128 devices in a mesh: io: 16 (over z, y), cmp: 8 (over x, core).
Axes of the slice: x: 4, y: 4, z: 4, core: 2. Of those that a mesh axis runs over, the one named last changes fastest.
Arguments:
- fields: float32 [6, 8, 1024, 4096], P(None, None, 'cmp', 'io'), may hold values from -6 to 6
- mean_old: float32 [6, 8, 1024, 3072], P(None, 'cmp', 'io'), may hold values from -6 to 6
- land_mask: int32 [8, 1024, 4096], P('cmp', 'io'), may hold values from 0 to 1, as said below
Outputs:
- mean_new: float32 [6, 8, 1024, 3072], P(None, 'cmp', 'io')
- level_rms: float32 [6, 8], P(None, 'cmp')
The draws below stay inside these ranges and needn't reach their ends.
Inputs may be any that keep to these rules, and one draw needn't show every extreme that they name: `land_mask`: each row (level, latitude) has between 1 and 3072 ocean points, and some row has exactly 3072.
All inputs are finite; a program needn't handle non-finite values.
Results may differ from the reference program's by a relative error of at most 0.00002.
Values sent between devices are 32-bit elements; how exact they have to be, the bound alone decides.
No kernel may reach another device: no remote copies, remote signals or barrier semaphores. Data moves between devices by JAX's collectives and lax.ppermute only.
A program may use at most 128 MiB of HBM per device.

```python
import jax
import jax.numpy as jnp
from jax import lax

FIELDS = 6
NI = 4096
L = 8
STEPS = 3
NJ = 1024
W = 3072


def draw_land_mask(key, part):
    key_scale, key_lev, key_row, key_perm = jax.random.split(jax.random.fold_in(key, 17), 4)
    row_index = jnp.arange(NJ, dtype=jnp.int32)
    base = W * (NJ + 3 * row_index) // (4 * NJ)
    factor = jax.random.randint(key_scale, (L, NJ), 80, 101)
    counts = jnp.maximum(base[None, :] * factor // 100, 1)
    pick_level = jax.random.randint(key_lev, (), 0, L)
    pick_row = jax.random.randint(key_row, (), 0, NJ)
    chosen = (jnp.arange(L, dtype=jnp.int32)[:, None] == pick_level) & (row_index[None, :] == pick_row)
    counts = jnp.where(chosen, W, counts)
    order = jnp.broadcast_to(jnp.arange(NI, dtype=jnp.int32), (L, NJ, NI))
    shuffled = jax.random.permutation(key_perm, order, axis=-1, independent=True)
    return (shuffled < counts[:, :, None]).astype(jnp.int32)


def shard_levels(own_key, shape, cuts, least, top_value):
    level = 1.0
    for dim, blocks in cuts:
        steps = jax.random.uniform(jax.random.fold_in(jax.random.fold_in(own_key, 6), dim), (blocks,), jnp.float32, least / len(cuts), top_value / len(cuts))
        level = level * jnp.repeat(jnp.exp(steps), shape[dim] // blocks).reshape((-1,) + (1,) * (len(shape) - 1 - dim))
    return level


def noise(stream_key, shape, spread, bound, cuts=(), kind=jnp.bfloat16):
    drawn = spread * jax.random.normal(stream_key, shape, jnp.float32)
    if cuts:
        drawn = drawn * shard_levels(stream_key, shape, cuts, -0.22, 0.18)
    return jnp.clip(drawn, -bound, bound).astype(kind)


def setup_inputs(seed: int = 0) -> dict:
    key_of = jax.random.split(jax.random.key(seed), 4)
    fields = noise(key_of[0], (FIELDS, L, NJ, NI), 1.0, 6.0, ((2, 8), (3, 16)), jnp.float32)
    mean_old = noise(key_of[1], (FIELDS, L, NJ, W), 1.0, 6.0, ((1, 8), (2, 16)), jnp.float32)
    land_mask = draw_land_mask(jax.random.fold_in(key_of[3], 71), 0)
    return dict(fields=fields, mean_old=mean_old, land_mask=land_mask)


def pack_one(values, target):
    width_out = 3 * values.shape[-1] // 4
    return jnp.zeros((values.shape[0], width_out), jnp.float32).at[:, target].set(values, mode='drop')

def pack_fields(fields, land_mask):
    nfield, nlev, nrow, ncol = fields.shape
    width_out = 3 * ncol // 4
    position = (jnp.cumsum(land_mask, axis=-1) - 1).astype(jnp.int32)
    target = jnp.where(land_mask == 1, position, width_out).astype(jnp.int32)
    flat = fields.reshape(nfield, nlev * nrow, ncol)
    packed = jax.vmap(pack_one, in_axes=(1, 0), out_axes=1)(flat, target.reshape(nlev * nrow, ncol))
    return packed.reshape(nfield, nlev, nrow, width_out)

def reference(fields, mean_old, land_mask):
    packed = pack_fields(fields, land_mask)
    counts = lax.optimization_barrier(jnp.sum(land_mask, axis=-1)).astype(jnp.int32)
    in_row = jnp.arange(mean_old.shape[-1], dtype=jnp.int32)[None, None, :] < counts[:, :, None]
    mean_new = jnp.where(in_row[None], (STEPS * mean_old + packed) / (STEPS + 1.0), jnp.float32(0.0))
    square_sum = lax.optimization_barrier(jnp.sum(mean_new * mean_new, axis=(2, 3)))
    ocean_total = lax.optimization_barrier(jnp.sum(counts, axis=1)).astype(jnp.float32)
    level_rms = jnp.sqrt(square_sum / ocean_total[None, :] + 1e-06)
    return (mean_new, level_rms)
```

```python
import jax
import jax.numpy as jnp
from jax import lax
from jax.experimental import pallas as pl
from jax.experimental.pallas import tpu as pltpu
from jax.sharding import PartitionSpec as P

STEPS = 3
LANES = 128
SUB = 8
ROUNDS = (
    (0, 0, 0), (2, 0, 1), (1, 1, 0), (3, 1, 1),
    (1, 0, 0), (3, 0, 1), (0, 1, 0), (2, 1, 1),
    (2, 0, 0), (0, 0, 1), (3, 1, 0), (1, 1, 1),
    (3, 0, 0), (1, 0, 1), (2, 1, 0), (0, 1, 1),
)


def target_of(i, c, rnd):
    kx, ks, kc = rnd
    z, y, x, _ = i >> 2, i & 3, c >> 1, c & 1
    level = ((x - z + kx) & 3) * 2 + ((y >> 1) ^ kc)
    half = (y & 1) ^ ks
    return level, half


def source_block(b, l, rnd):
    kx, ks, kc = rnd
    z1, y1, x1, core1 = b >> 2, b & 3, l >> 1, l & 1
    z = (z1 - x1 + kx) & 3
    return z * 4 + (core1 ^ kc) * 2 + ((y1 & 1) ^ ks)


def pairs_of(rnd):
    out = []
    for i in range(16):
        for c in range(8):
            level, half = target_of(i, c, rnd)
            out.append((i * 8 + c, (2 * c + half) * 8 + level))
    return out


def index_kernel(mask_ref, lane_ref, move_ref, count_ref, dist_ref):
    rows, ncol = mask_ref.shape
    chunks = ncol // LANES
    before = lax.broadcasted_iota(jnp.int32, (LANES, LANES), 0) <= lax.broadcasted_iota(
        jnp.int32, (LANES, LANES), 1
    )
    upper = before.astype(jnp.bfloat16)
    ones = jnp.ones((LANES, LANES), jnp.bfloat16)
    lane = lax.broadcasted_iota(jnp.int32, (rows, LANES), 1)
    start = jnp.zeros((rows, LANES), jnp.int32)
    for k in range(chunks):
        cut = slice(k * LANES, (k + 1) * LANES)
        mask = mask_ref[:, cut]
        ocean = mask == 1
        mb = mask.astype(jnp.float32).astype(jnp.bfloat16)
        upto = jnp.dot(mb, upper, preferred_element_type=jnp.float32).astype(jnp.int32)
        total = jnp.dot(mb, ones, preferred_element_type=jnp.float32).astype(jnp.int32)
        state = jnp.where(ocean, ((lane - upto + 1) << 7) | lane, 0)
        for bit in range(7):
            moving = jnp.where((state >> (7 + bit)) & 1 == 1, state, 0)
            state = (state ^ moving) | pltpu.roll(moving, LANES - (1 << bit), 1)
        rank = (lane - start) & (LANES - 1)
        lane_ref[:, cut] = jnp.take_along_axis(state & (LANES - 1), rank, axis=1)
        chunk = (start + rank) >> 7
        dist_ref[:, cut] = jnp.where(rank < total, k - chunk, 0)
        start = start + total
    count_ref[...] = start
    for k in range(chunks):
        move_ref[:, k * LANES : (k + 1) * LANES] = jnp.zeros((rows, LANES), jnp.int32)
    for bit in range(5):
        amount = 1 << bit
        for k in range(chunks):
            cut = slice(k * LANES, (k + 1) * LANES)
            here = dist_ref[:, cut]
            stay = jnp.where((here >> bit) & 1 == 1, 0, here)
            if k + amount < chunks:
                there = dist_ref[:, (k + amount) * LANES : (k + amount + 1) * LANES]
                arrive = (there >> bit) & 1 == 1
                move_ref[:, cut] = move_ref[:, cut] | jnp.where(arrive, amount, 0)
                dist_ref[:, cut] = jnp.where(arrive, there, stay)
            else:
                dist_ref[:, cut] = stay


def pack_kernel(where_ref, lane_ref, move_ref, count_ref, old_ref, *refs):
    rounds = len(ROUNDS)
    pieces = refs[:rounds]
    new_ref, sum_ref, turned, out, sem = refs[rounds:]
    fields, rows, width = old_ref.shape
    chunks = lane_ref.shape[1] // LANES
    groups = rows // SUB
    wide = width // LANES
    lane = lax.broadcasted_iota(jnp.int32, (SUB, LANES), 1)

    def copy_out(g, slot):
        return pltpu.make_async_copy(
            out.at[slot], new_ref.at[:, pl.ds(pl.multiple_of(g * SUB, SUB), SUB), :], sem.at[slot]
        )

    def group(g, sums):
        slot = lax.rem(g, 2)
        band = pl.ds(pl.multiple_of(g * SUB, SUB), SUB)

        @pl.when(g >= 2)
        def _():
            copy_out(g - 2, slot).wait()

        count = count_ref[band, :]
        for r in range(rounds):
            first = where_ref[r] * 2
            for h in range(2):
                at = first + h
                index = lane_ref[band, pl.ds(pl.multiple_of(at * LANES, LANES), LANES)]
                for f in range(fields):
                    value = pieces[r][f, band, h * LANES : (h + 1) * LANES]
                    turned[f, at] = jnp.take_along_axis(value, index, axis=1)
        sums = list(sums)
        for f in range(fields):
            values = [turned[f, k] for k in range(chunks)]
            for bit in range(5):
                amount = 1 << bit
                for k in range(chunks - amount):
                    arrive = (move_ref[band, k * LANES : (k + 1) * LANES] & amount) != 0
                    values[k] = jnp.where(arrive, values[k + amount], values[k])
            for k in range(wide):
                old = old_ref[f, band, k * LANES : (k + 1) * LANES]
                mean = (STEPS * old + values[k]) * (1.0 / (STEPS + 1.0))
                mean = jnp.where(lane + k * LANES < count, mean, 0.0)
                out[slot, f, :, k * LANES : (k + 1) * LANES] = mean
                sums[f] = sums[f] + mean * mean
        copy_out(g, slot).start()
        return tuple(sums)

    zero = jnp.zeros((SUB, LANES), jnp.float32)
    sums = lax.fori_loop(0, groups, group, (zero,) * fields)
    row = lax.broadcasted_iota(jnp.int32, (SUB, LANES), 0)
    total = zero
    for f in range(fields):
        total = jnp.where(row == f, jnp.sum(sums[f]), total)
    ocean = jnp.sum(jnp.where(lane[:1] == 0, count_ref[...], 0).astype(jnp.float32))
    sum_ref[...] = jnp.where(row == fields, ocean, total)
    for g in range(groups - 2, groups):
        copy_out(g, g % 2).wait()


VMEM = pl.BlockSpec(memory_space=pltpu.VMEM)


def row_indices(mask):
    rows, ncol = mask.shape
    full = jax.ShapeDtypeStruct((rows, ncol), jnp.int32)
    return pl.pallas_call(
        index_kernel,
        out_shape=(full, full, jax.ShapeDtypeStruct((rows, LANES), jnp.int32)),
        in_specs=[VMEM],
        out_specs=(VMEM, VMEM, VMEM),
        scratch_shapes=[pltpu.VMEM((rows, ncol), jnp.int32)],
        compiler_params=pltpu.CompilerParams(vmem_limit_bytes=16 << 20),
        cost_estimate=pl.CostEstimate(flops=20_000_000, bytes_accessed=4 << 20, transcendentals=0),
        name="row_indices",
    )(mask)


def pack(where, lanes, moves, counts, old, pieces):
    fields, rows, width = old.shape
    chunks = lanes.shape[1] // LANES
    return pl.pallas_call(
        pack_kernel,
        out_shape=(
            jax.ShapeDtypeStruct(old.shape, jnp.float32),
            jax.ShapeDtypeStruct((SUB, LANES), jnp.float32),
        ),
        in_specs=[pl.BlockSpec(memory_space=pltpu.SMEM)] + [VMEM] * (4 + len(pieces)),
        out_specs=(pl.BlockSpec(memory_space=pl.ANY), VMEM),
        scratch_shapes=[
            pltpu.VMEM((fields, chunks, SUB, LANES), jnp.float32),
            pltpu.VMEM((2, fields, SUB, width), jnp.float32),
            pltpu.SemaphoreType.DMA((2,)),
        ],
        compiler_params=pltpu.CompilerParams(vmem_limit_bytes=40 << 20),
        cost_estimate=pl.CostEstimate(flops=40_000_000, bytes_accessed=16 << 20, transcendentals=0),
        name="pack",
    )(where, lanes, moves, counts, old, *pieces)


def over_copies(value, axis):
    devices = lax.axis_size(axis)
    sent = jnp.broadcast_to(value[None], (devices, *value.shape))
    return lax.all_to_all(sent, axis, 0, 0, tiled=True).sum(axis=0)


def on_device(fields, mean_old, land_mask):
    nfield, _, nrow, ncol = fields.shape
    i, c = lax.axis_index("io"), lax.axis_index("cmp")
    band = nrow // 2
    pieces = []
    for rnd in ROUNDS:
        level, half = target_of(i, c, rnd)
        piece = lax.dynamic_slice(fields, (0, level, half * band, 0), (nfield, 1, band, ncol))
        pieces.append(lax.ppermute(piece[:, 0], ("io", "cmp"), pairs_of(rnd)))
    lanes, moves, counts = row_indices(land_mask[0])
    where = jnp.stack([source_block(i, c, rnd) for rnd in ROUNDS]).astype(jnp.int32)
    mean_new, part = pack(where, lanes, moves, counts, mean_old[:, 0], pieces)
    total = over_copies(part[: nfield + 1, 0], "io")
    level_rms = jnp.sqrt(total[:nfield] / total[nfield] + 1e-06)
    return mean_new[:, None], level_rms[:, None]


def solution(mesh):
    in_specs = (P(None, None, "cmp", "io"), P(None, "cmp", "io", None), P("cmp", "io", None))
    out_specs = (P(None, "cmp", "io", None), P(None, "cmp"))
    return jax.shard_map(
        on_device, mesh=mesh, in_specs=in_specs, out_specs=out_specs, check_vma=False
    )
```

```python
import jax
import jax.numpy as jnp
from jax import lax
from jax.experimental import pallas as pl
from jax.experimental.pallas import tpu as pltpu
from jax.sharding import PartitionSpec as P


STEPS = 3
LANES = 128
SUB = 8
ROUNDS = tuple(
    (kx, ks, kc) for kc in (0, 1) for pair in ((1, 3), (0, 2)) for ks in (1, 0) for kx in pair
)
STAGES = 5


def target_of(i, c, rnd):
    kx, ks, kc = rnd
    z, y, x = i >> 2, i & 3, c >> 1
    level = ((x - z + kx) & 3) * 2 + ((y >> 1) ^ kc)
    half = (y & 1) ^ ks
    return level, half


def source_block(b, l, rnd):
    kx, ks, kc = rnd
    z1, y1, x1, core1 = b >> 2, b & 3, l >> 1, l & 1
    z = (z1 - x1 + kx) & 3
    return z * 4 + (core1 ^ kc) * 2 + ((y1 & 1) ^ ks)


def pairs_of(rnd):
    out = []
    for i in range(16):
        for c in range(8):
            level, half = target_of(i, c, rnd)
            out.append((i * 8 + c, (2 * c + half) * 8 + level))
    return out


def cut_kernel(fields_ref, *refs):
    rounds = len(ROUNDS)
    outs, sem = refs[:rounds], refs[rounds]
    rows = outs[0].shape[1]
    i, c = lax.axis_index("io"), lax.axis_index("cmp")
    copies = []
    for r, rnd in enumerate(ROUNDS):
        level, half = target_of(i, c, rnd)
        band = pl.ds(pl.multiple_of(half * rows, rows), rows)
        copies.append(
            pltpu.make_async_copy(fields_ref.at[:, level, band, :], outs[r], sem.at[r])
        )
    for copy in copies:
        copy.start()
    for copy in copies:
        copy.wait()


def lane_gather(values, index):
    return jnp.take_along_axis(values, index, axis=1, mode="promise_in_bounds")


def index_kernel(mask_ref, lane_ref, move_ref, count_ref, dist_ref):
    rows, ncol = mask_ref.shape
    chunks = ncol // LANES
    before = lax.broadcasted_iota(jnp.int32, (LANES, LANES), 0) <= lax.broadcasted_iota(
        jnp.int32, (LANES, LANES), 1
    )
    upper = before.astype(jnp.bfloat16)
    ones = jnp.ones((LANES, LANES), jnp.bfloat16)
    lane = lax.broadcasted_iota(jnp.int32, (rows, LANES), 1)
    start = jnp.zeros((rows, LANES), jnp.int32)
    for k in range(chunks):
        cut = slice(k * LANES, (k + 1) * LANES)
        mask = mask_ref[:, cut]
        ocean = mask == 1
        mb = mask.astype(jnp.float32).astype(jnp.bfloat16)
        upto = jnp.dot(mb, upper, preferred_element_type=jnp.float32).astype(jnp.int32)
        total = jnp.dot(mb, ones, preferred_element_type=jnp.float32).astype(jnp.int32)
        state = jnp.where(ocean, ((lane - upto + 1) << 7) | lane, 0)
        for bit in range(7):
            moving = jnp.where((state >> (7 + bit)) & 1 == 1, state, 0)
            state = (state ^ moving) | pltpu.roll(moving, LANES - (1 << bit), 1)
        rank = (lane - start) & (LANES - 1)
        lane_ref[:, cut] = lane_gather(state & (LANES - 1), rank)
        chunk = (start + rank) >> 7
        dist_ref[:, cut] = jnp.where(rank < total, k - chunk, 0)
        start = start + total
    count_ref[...] = start
    for bit in range(STAGES):
        amount = 1 << bit
        for k in range(chunks):
            cut = slice(k * LANES, (k + 1) * LANES)
            here = dist_ref[:, cut]
            stay = jnp.where((here >> bit) & 1 == 1, 0, here)
            if k + amount < chunks:
                there = dist_ref[:, (k + amount) * LANES : (k + amount + 1) * LANES]
                arrive = there & amount
                move_ref[bit, :, cut] = arrive
                dist_ref[:, cut] = jnp.where(arrive != 0, there, stay)
            else:
                dist_ref[:, cut] = stay


def pack_kernel(lane_ref, move_ref, count_ref, old_ref, *refs):
    rounds = len(ROUNDS)
    pieces = refs[:rounds]
    new_ref, sum_ref, turned, out, acc, sem = refs[rounds:]
    fields, rows, width = old_ref.shape
    chunks = lane_ref.shape[1] // LANES
    groups = rows // SUB
    wide = width // LANES
    lane = lax.broadcasted_iota(jnp.int32, (SUB, LANES), 1)
    acc[...] = jnp.zeros_like(acc)
    io, cmp = lax.axis_index("io"), lax.axis_index("cmp")

    def copy_out(g, slot):
        return pltpu.make_async_copy(
            out.at[slot], new_ref.at[:, pl.ds(pl.multiple_of(g * SUB, SUB), SUB), :], sem.at[slot]
        )

    @pl.loop(0, groups)
    def _(g):
        slot = lax.rem(g, 2)
        band = pl.ds(pl.multiple_of(g * SUB, SUB), SUB)

        @pl.when(g >= 2)
        def _():
            copy_out(g - 2, slot).wait()

        left = count_ref[band, :] - lane
        for r in range(rounds):
            first = source_block(io, cmp, ROUNDS[r]) * 2
            for h in range(2):
                at = first + h
                index = lane_ref[band, pl.ds(pl.multiple_of(at * LANES, LANES), LANES)]
                for f in range(fields):
                    value = pieces[r][f, band, h * LANES : (h + 1) * LANES]
                    turned[f, at] = lane_gather(value, index)

        @pl.loop(0, fields)
        def _(f):
            values = [turned[f, k] for k in range(chunks)]
            for bit in range(STAGES):
                amount = 1 << bit
                for k in range(chunks - amount):
                    if bit == STAGES - 1 and k >= wide:
                        continue
                    arrive = move_ref[bit, band, k * LANES : (k + 1) * LANES] != 0
                    values[k] = jnp.where(arrive, values[k + amount], values[k])
            squares = acc[f]
            for k in range(wide):
                old = old_ref[f, band, k * LANES : (k + 1) * LANES]
                mean = (STEPS * old + values[k]) * (1.0 / (STEPS + 1.0))
                mean = jnp.where(left > k * LANES, mean, 0.0)
                out[slot, f, :, k * LANES : (k + 1) * LANES] = mean
                squares = squares + mean * mean
            acc[f] = squares

        copy_out(g, slot).start()

    row = lax.broadcasted_iota(jnp.int32, (SUB, LANES), 0)
    total = jnp.zeros((SUB, LANES), jnp.float32)
    for f in range(fields):
        total = jnp.where(row == f, jnp.sum(acc[f]), total)
    ocean = jnp.sum(jnp.where(lane[:1] == 0, count_ref[...], 0).astype(jnp.float32))
    total = jnp.where(row == fields, ocean, total)
    for p in range(sum_ref.shape[0]):
        sum_ref[p] = total
    for g in range(groups - 2, groups):
        copy_out(g, g % 2).wait()


VMEM = pl.BlockSpec(memory_space=pltpu.VMEM)


def cut(fields):
    nfield, _, nrow, ncol = fields.shape
    rounds = len(ROUNDS)
    piece = jax.ShapeDtypeStruct((nfield, nrow // 2, ncol), jnp.float32)
    return pl.pallas_call(
        cut_kernel,
        out_shape=(piece,) * rounds,
        in_specs=[pl.BlockSpec(memory_space=pltpu.HBM)],
        out_specs=(VMEM,) * rounds,
        scratch_shapes=[pltpu.SemaphoreType.DMA((rounds,))],
        compiler_params=pltpu.CompilerParams(vmem_limit_bytes=46 << 20),
        cost_estimate=pl.CostEstimate(flops=0, bytes_accessed=12 << 20, transcendentals=0),
        name="cut",
    )(fields)


def row_indices(mask):
    rows, ncol = mask.shape
    return pl.pallas_call(
        index_kernel,
        out_shape=(
            jax.ShapeDtypeStruct((rows, ncol), jnp.int32),
            jax.ShapeDtypeStruct((STAGES, rows, ncol), jnp.int32),
            jax.ShapeDtypeStruct((rows, LANES), jnp.int32),
        ),
        in_specs=[VMEM],
        out_specs=(VMEM, VMEM, VMEM),
        scratch_shapes=[pltpu.VMEM((rows, ncol), jnp.int32)],
        compiler_params=pltpu.CompilerParams(vmem_limit_bytes=3 << 20),
        cost_estimate=pl.CostEstimate(flops=20_000_000, bytes_accessed=12 << 20, transcendentals=0),
        name="row_indices",
    )(mask)


def pack(lanes, moves, counts, old, pieces, copies=16):
    fields, _, width = old.shape
    chunks = lanes.shape[1] // LANES
    return pl.pallas_call(
        pack_kernel,
        out_shape=(
            jax.ShapeDtypeStruct(old.shape, jnp.float32),
            jax.ShapeDtypeStruct((copies, SUB, LANES), jnp.float32),
        ),
        in_specs=[VMEM] * (4 + len(pieces)),
        out_specs=(pl.BlockSpec(memory_space=pltpu.HBM), VMEM),
        scratch_shapes=[
            pltpu.VMEM((fields, chunks, SUB, LANES), jnp.float32),
            pltpu.VMEM((2, fields, SUB, width), jnp.float32),
            pltpu.VMEM((fields, SUB, LANES), jnp.float32),
            pltpu.SemaphoreType.DMA((2,)),
        ],
        compiler_params=pltpu.CompilerParams(vmem_limit_bytes=12 << 20),
        cost_estimate=pl.CostEstimate(flops=40_000_000, bytes_accessed=16 << 20, transcendentals=0),
        name="pack",
    )(lanes, moves, counts, old, *pieces)


def on_device(fields, mean_old, land_mask):
    nfield = fields.shape[0]
    cuts = cut(fields)
    pieces = []
    for k, rnd in enumerate(ROUNDS):
        pieces.append(lax.ppermute(cuts[k], ("io", "cmp"), pairs_of(rnd)))
    lanes, moves, counts = row_indices(land_mask[0])
    mean_new, part = pack(lanes, moves, counts, mean_old[:, 0], pieces, lax.axis_size("io"))
    total = lax.all_to_all(part, "io", 0, 0, tiled=True)[:, : nfield + 1, :1].sum(axis=0)
    level_rms = jnp.sqrt(total[:nfield] / total[nfield] + 1e-06)
    return mean_new[:, None], level_rms


def solution(mesh):
    in_specs = (P(None, None, "cmp", "io"), P(None, "cmp", "io", None), P("cmp", "io", None))
    out_specs = (P(None, "cmp", "io", None), P(None, "cmp"))
    return jax.shard_map(
        on_device, mesh=mesh, in_specs=in_specs, out_specs=out_specs, check_vma=False
    )
```

```python
import functools

import jax
import jax.numpy as jnp
from jax import lax
from jax.experimental import pallas as pl
from jax.experimental.pallas import tpu as pltpu
from jax.sharding import PartitionSpec as P


STEPS = 3
LANES = 128
SUB = 8
ROUNDS = tuple(
    (kx, ks, kc) for pair in ((1, 3), (0, 2)) for ks in (1, 0) for kc in (0, 1) for kx in pair
)
STAGES = 5
TURNS = (0, 8, 13, 16)
SHARE = 3


def target_of(i, c, rnd):
    kx, ks, kc = rnd
    z, y, x = i >> 2, i & 3, c >> 1
    level = ((x - z + kx) & 3) * 2 + ((y >> 1) ^ kc)
    half = (y & 1) ^ ks
    return level, half


def source_block(b, l, rnd):
    kx, ks, kc = rnd
    z1, y1, x1, core1 = b >> 2, b & 3, l >> 1, l & 1
    z = (z1 - x1 + kx) & 3
    return z * 4 + (core1 ^ kc) * 2 + ((y1 & 1) ^ ks)


def pairs_of(rnd):
    out = []
    for i in range(16):
        for c in range(8):
            level, half = target_of(i, c, rnd)
            out.append((i * 8 + c, (2 * c + half) * 8 + level))
    return out


def cut_kernel(fields_ref, *refs):
    rounds = len(ROUNDS)
    outs, sem = refs[:rounds], refs[rounds]
    rows = outs[0].shape[1]
    i, c = lax.axis_index("io"), lax.axis_index("cmp")
    copies = []
    for r, rnd in enumerate(ROUNDS):
        level, half = target_of(i, c, rnd)
        band = pl.ds(pl.multiple_of(half * rows, rows), rows)
        copies.append(
            pltpu.make_async_copy(fields_ref.at[:, level, band, :], outs[r], sem.at[r])
        )
    for copy in copies:
        copy.start()
    for copy in copies:
        copy.wait()


def lane_gather(values, index):
    return jnp.take_along_axis(values, index, axis=1, mode="promise_in_bounds")


def index_kernel(mask_ref, old_ref, lane_ref, move_ref, count_ref, share_ref, dist_ref):
    rows, ncol = mask_ref.shape
    chunks = ncol // LANES
    before = lax.broadcasted_iota(jnp.int32, (LANES, LANES), 0) <= lax.broadcasted_iota(
        jnp.int32, (LANES, LANES), 1
    )
    upper = before.astype(jnp.bfloat16)
    ones = jnp.ones((LANES, LANES), jnp.bfloat16)
    lane = lax.broadcasted_iota(jnp.int32, (rows, LANES), 1)
    start = jnp.zeros((rows, LANES), jnp.int32)
    for k in range(chunks):
        cut = slice(k * LANES, (k + 1) * LANES)
        mask = mask_ref[:, cut]
        ocean = mask == 1
        mb = mask.astype(jnp.float32).astype(jnp.bfloat16)
        upto = jnp.dot(mb, upper, preferred_element_type=jnp.float32).astype(jnp.int32)
        total = jnp.dot(mb, ones, preferred_element_type=jnp.float32).astype(jnp.int32)
        state = jnp.where(ocean, ((lane - upto + 1) << 7) | lane, 0)
        for bit in range(7):
            moving = jnp.where((state >> (7 + bit)) & 1 == 1, state, 0)
            state = (state ^ moving) | pltpu.roll(moving, LANES - (1 << bit), 1)
        rank = (lane - start) & (LANES - 1)
        lane_ref[:, cut] = lane_gather(state & (LANES - 1), rank)
        chunk = (start + rank) >> 7
        dist_ref[:, cut] = jnp.where(rank < total, k - chunk, 0)
        start = start + total
    count_ref[...] = start
    for f in range(old_ref.shape[0]):
        share_ref[f] = old_ref[f] * (STEPS / (STEPS + 1.0))
    for bit in range(STAGES):
        amount = 1 << bit
        for k in range(chunks):
            cut = slice(k * LANES, (k + 1) * LANES)
            here = dist_ref[:, cut]
            stay = jnp.where((here >> bit) & 1 == 1, 0, here)
            if k + amount < chunks:
                there = dist_ref[:, (k + amount) * LANES : (k + amount + 1) * LANES]
                arrive = there & amount
                move_ref[bit, :, cut] = arrive
                dist_ref[:, cut] = jnp.where(arrive != 0, there, stay)
            else:
                dist_ref[:, cut] = stay


def turn_kernel(rounds, reuse, lane_ref, *refs):
    pieces = refs[: len(rounds)]
    turned = refs[len(rounds) + reuse]
    fields, rows, _ = pieces[0].shape
    io, cmp = lax.axis_index("io"), lax.axis_index("cmp")

    @pl.loop(0, rows // SUB)
    def _(g):
        band = pl.ds(pl.multiple_of(g * SUB, SUB), SUB)
        for r, rnd in enumerate(rounds):
            first = source_block(io, cmp, rnd) * 2
            for h in range(2):
                at = first + h
                index = lane_ref[band, pl.ds(pl.multiple_of(at * LANES, LANES), LANES)]
                for f in range(fields):
                    value = pieces[r][f, band, h * LANES : (h + 1) * LANES]
                    turned[f, at, band, :] = lane_gather(value, index) * (1.0 / (STEPS + 1.0))


def moved_chunks(turned, move_ref, fs, band, wide):
    chunks = turned.shape[1]
    level = [{} for _ in range(STAGES + 1)]

    def settle(bit, k):
        if bit == STAGES:
            return
        amount = 1 << bit
        for at in (k - amount, k):
            if at < 0 or at in level[bit + 1] or (at + amount < chunks and at == k):
                continue
            value = level[bit].pop(at)
            if at + amount < chunks:
                arrive = move_ref[bit, band, at * LANES : (at + 1) * LANES] != 0
                near = level[bit][at + amount]
                value = [jnp.where(arrive, n, v) for n, v in zip(near, value)]
            level[bit + 1][at] = value
            settle(bit + 1, at)

    done = 0
    for k in range(chunks):
        level[0][k] = [turned[f, k, band, :] for f in fs]
        settle(0, k)
        while done < wide and done in level[STAGES]:
            yield done, level[STAGES].pop(done)
            level[STAGES][done] = None
            done += 1


def pack_kernel(turned, move_ref, count_ref, old_ref, new_ref, sum_ref, out, acc, sem):
    fields, rows, width = old_ref.shape
    groups = rows // SUB
    wide = width // LANES
    lane = lax.broadcasted_iota(jnp.int32, (SUB, LANES), 1)
    acc[...] = jnp.zeros_like(acc)

    def copy_out(g, slot):
        return pltpu.make_async_copy(
            out.at[slot], new_ref.at[:, pl.ds(pl.multiple_of(g * SUB, SUB), SUB), :], sem.at[slot]
        )

    @pl.loop(0, groups)
    def _(g):
        slot = lax.rem(g, 2)
        band = pl.ds(pl.multiple_of(g * SUB, SUB), SUB)

        @pl.when(g >= 2)
        def _():
            copy_out(g - 2, slot).wait()

        left = count_ref[band, :] - lane

        @pl.loop(0, fields, step=SHARE)
        def _(f0):
            fs = [f0 + j for j in range(SHARE)]
            squares = [acc[f] for f in fs]
            for k, values in moved_chunks(turned, move_ref, fs, band, wide):
                valid = left > k * LANES
                cut = slice(k * LANES, (k + 1) * LANES)
                for j, f in enumerate(fs):
                    mean = jnp.where(valid, old_ref[f, band, cut] + values[j], 0.0)
                    out[slot, f, :, cut] = mean
                    squares[j] = squares[j] + mean * mean
            for j, f in enumerate(fs):
                acc[f] = squares[j]

        copy_out(g, slot).start()

    row = lax.broadcasted_iota(jnp.int32, (SUB, LANES), 0)
    total = jnp.zeros((SUB, LANES), jnp.float32)
    for f in range(fields):
        total = jnp.where(lane == f, jnp.sum(acc[f]), total)
    ocean = jnp.sum(jnp.where(lane[:1] == 0, count_ref[...], 0).astype(jnp.float32))
    total = jnp.where(row == 1, ocean, total)
    for p in range(sum_ref.shape[0]):
        sum_ref[p] = total
    for g in range(groups - 2, groups):
        copy_out(g, g % 2).wait()


def finish_kernel(part_ref, rms_ref):
    total = part_ref[0]
    for p in range(1, part_ref.shape[0]):
        total = total + part_ref[p]
    rms = jnp.sqrt(total[0:1] / total[1:2] + 1e-06)
    rms_ref[...] = rms[:, : rms_ref.shape[1]]


VMEM = pl.BlockSpec(memory_space=pltpu.VMEM)


def cut(fields):
    nfield, _, nrow, ncol = fields.shape
    rounds = len(ROUNDS)
    piece = jax.ShapeDtypeStruct((nfield, nrow // 2, ncol), jnp.float32)
    return pl.pallas_call(
        cut_kernel,
        out_shape=(piece,) * rounds,
        in_specs=[pl.BlockSpec(memory_space=pltpu.HBM)],
        out_specs=(VMEM,) * rounds,
        scratch_shapes=[pltpu.SemaphoreType.DMA((rounds,))],
        compiler_params=pltpu.CompilerParams(vmem_limit_bytes=46 << 20),
        cost_estimate=pl.CostEstimate(flops=0, bytes_accessed=12 << 20, transcendentals=0),
        name="cut",
    )(fields)


def row_indices(mask, old):
    rows, ncol = mask.shape
    return pl.pallas_call(
        index_kernel,
        out_shape=(
            jax.ShapeDtypeStruct((rows, ncol), jnp.int32),
            jax.ShapeDtypeStruct((STAGES, rows, ncol), jnp.int32),
            jax.ShapeDtypeStruct((rows, LANES), jnp.int32),
            jax.ShapeDtypeStruct(old.shape, jnp.float32),
        ),
        in_specs=[VMEM, VMEM],
        out_specs=(VMEM,) * 4,
        scratch_shapes=[pltpu.VMEM((rows, ncol), jnp.int32)],
        compiler_params=pltpu.CompilerParams(vmem_limit_bytes=3 << 20),
        cost_estimate=pl.CostEstimate(flops=20_000_000, bytes_accessed=12 << 20, transcendentals=0),
        name="row_indices",
    )(mask, old)


def turn(rounds, lanes, pieces, turned):
    fields, rows, _ = pieces[0].shape
    shape = jax.ShapeDtypeStruct((fields, lanes.shape[1] // LANES, rows, LANES), jnp.float32)
    before = [] if turned is None else [turned]
    return pl.pallas_call(
        functools.partial(turn_kernel, rounds, len(before)),
        out_shape=shape,
        in_specs=[VMEM] * (1 + len(pieces) + len(before)),
        out_specs=VMEM,
        input_output_aliases={1 + len(pieces): 0} if before else {},
        compiler_params=pltpu.CompilerParams(vmem_limit_bytes=2 << 20),
        cost_estimate=pl.CostEstimate(
            flops=1_000_000 * len(pieces), bytes_accessed=800_000 * len(pieces), transcendentals=0
        ),
        name="turn",
    )(lanes, *pieces, *before)


def pack(turned, moves, counts, old, copies=16):
    fields, _, width = old.shape
    return pl.pallas_call(
        pack_kernel,
        out_shape=(
            jax.ShapeDtypeStruct(old.shape, jnp.float32),
            jax.ShapeDtypeStruct((copies, SUB, LANES), jnp.float32),
        ),
        in_specs=[VMEM] * 4,
        out_specs=(pl.BlockSpec(memory_space=pltpu.HBM), VMEM),
        scratch_shapes=[
            pltpu.VMEM((2, fields, SUB, width), jnp.float32),
            pltpu.VMEM((fields, SUB, LANES), jnp.float32),
            pltpu.SemaphoreType.DMA((2,)),
        ],
        compiler_params=pltpu.CompilerParams(vmem_limit_bytes=6 << 20),
        cost_estimate=pl.CostEstimate(flops=40_000_000, bytes_accessed=16 << 20, transcendentals=0),
        name="pack",
    )(turned, moves, counts, old)


def finish(part, fields):
    return pl.pallas_call(
        finish_kernel,
        out_shape=jax.ShapeDtypeStruct((1, fields), jnp.float32),
        in_specs=[VMEM],
        out_specs=VMEM,
        compiler_params=pltpu.CompilerParams(vmem_limit_bytes=1 << 20),
        name="finish",
    )(part)


def on_device(fields, mean_old, land_mask):
    nfield = fields.shape[0]
    cuts = cut(fields)
    pieces = []
    for k, rnd in enumerate(ROUNDS):
        pieces.append(lax.ppermute(cuts[k], ("io", "cmp"), pairs_of(rnd)))
    lanes, moves, counts, share = row_indices(land_mask[0], mean_old[:, 0])
    turned = None
    for low, high in zip(TURNS, TURNS[1:]):
        turned = turn(ROUNDS[low:high], lanes, pieces[low:high], turned)
    mean_new, part = pack(turned, moves, counts, share, lax.axis_size("io"))
    rms = finish(lax.all_to_all(part, "io", 0, 0, tiled=True), nfield)
    return mean_new[:, None], rms.T


def solution(mesh):
    in_specs = (P(None, None, "cmp", "io"), P(None, "cmp", "io", None), P("cmp", "io", None))
    out_specs = (P(None, "cmp", "io", None), P(None, "cmp"))
    return jax.shard_map(
        on_device, mesh=mesh, in_specs=in_specs, out_specs=out_specs, check_vma=False
    )
```

```python
import functools

import jax
import jax.numpy as jnp
from jax import lax
from jax.experimental import pallas as pl
from jax.experimental.pallas import tpu as pltpu
from jax.sharding import PartitionSpec as P


STEPS = 3
LANES = 128
SUB = 8
ROUNDS = tuple(
    (pair[j ^ kc], ks, kc)
    for pair in ((1, 3), (0, 2))
    for ks in (1, 0)
    for kc in (0, 1)
    for j in (0, 1)
)
STAGES = 5
TURNS = (0, 8, 13, 15, 16)
CUTS = (0, 4, 16)
GRANTS = (204, 192)
SHARE = 2


def target_of(i, c, rnd):
    kx, ks, kc = rnd
    z, y, x = i >> 2, i & 3, c >> 1
    level = ((x - z + kx) & 3) * 2 + ((y >> 1) ^ kc)
    half = (y & 1) ^ ks
    return level, half


def source_block(b, l, rnd):
    kx, ks, kc = rnd
    z1, y1, x1, core1 = b >> 2, b & 3, l >> 1, l & 1
    z = (z1 - x1 + kx) & 3
    return z * 4 + (core1 ^ kc) * 2 + ((y1 & 1) ^ ks)


def pairs_of(rnd):
    out = []
    for i in range(16):
        for c in range(8):
            level, half = target_of(i, c, rnd)
            out.append((i * 8 + c, (2 * c + half) * 8 + level))
    return out


def cut_kernel(rounds, fields_ref, *refs):
    outs, sem = refs[: len(rounds)], refs[len(rounds)]
    rows = outs[0].shape[1]
    i, c = lax.axis_index("io"), lax.axis_index("cmp")
    copies = []
    for r, rnd in enumerate(rounds):
        level, half = target_of(i, c, rnd)
        band = pl.ds(pl.multiple_of(half * rows, rows), rows)
        copies.append(
            pltpu.make_async_copy(fields_ref.at[:, level, band, :], outs[r], sem.at[r])
        )
    for copy in copies:
        copy.start()
    for copy in copies:
        copy.wait()


def lane_gather(values, index):
    return jnp.take_along_axis(values, index, axis=1, mode="promise_in_bounds")


def index_kernel(mask_ref, old_ref, lane_ref, move_ref, count_ref, share_ref, dist_ref):
    rows, ncol = mask_ref.shape
    chunks = ncol // LANES
    before = lax.broadcasted_iota(jnp.int32, (LANES, LANES), 0) <= lax.broadcasted_iota(
        jnp.int32, (LANES, LANES), 1
    )
    upper = before.astype(jnp.bfloat16)
    ones = jnp.ones((LANES, LANES), jnp.bfloat16)
    lane = lax.broadcasted_iota(jnp.int32, (rows, LANES), 1)
    start = jnp.zeros((rows, LANES), jnp.int32)
    for k in range(chunks):
        cut = slice(k * LANES, (k + 1) * LANES)
        mask = mask_ref[:, cut]
        ocean = mask == 1
        mb = mask.astype(jnp.float32).astype(jnp.bfloat16)
        upto = jnp.dot(mb, upper, preferred_element_type=jnp.float32).astype(jnp.int32)
        total = jnp.dot(mb, ones, preferred_element_type=jnp.float32).astype(jnp.int32)
        state = jnp.where(ocean, ((lane - upto + 1) << 7) | lane, 0)
        for bit in range(7):
            moving = jnp.where((state >> (7 + bit)) & 1 == 1, state, 0)
            state = (state ^ moving) | pltpu.roll(moving, LANES - (1 << bit), 1)
        rank = (lane - start) & (LANES - 1)
        lane_ref[:, cut] = lane_gather(state & (LANES - 1), rank)
        chunk = (start + rank) >> 7
        dist_ref[:, cut] = jnp.where(rank < total, k - chunk, 0)
        start = start + total
    count_ref[...] = start
    for f in range(old_ref.shape[0]):
        share_ref[f] = old_ref[f] * (STEPS / (STEPS + 1.0))
    for bit in range(STAGES):
        amount = 1 << bit
        for k in range(chunks):
            cut = slice(k * LANES, (k + 1) * LANES)
            here = dist_ref[:, cut]
            stay = jnp.where((here >> bit) & 1 == 1, 0, here)
            if k + amount < chunks:
                there = dist_ref[:, (k + amount) * LANES : (k + amount + 1) * LANES]
                arrive = there & amount
                move_ref[bit, :, cut] = arrive
                dist_ref[:, cut] = jnp.where(arrive != 0, there, stay)
            else:
                dist_ref[:, cut] = stay


def turn_kernel(rounds, reuse, lane_ref, *refs):
    pieces = refs[: len(rounds)]
    turned = refs[len(rounds) + reuse]
    fields, rows, _ = pieces[0].shape
    io, cmp = lax.axis_index("io"), lax.axis_index("cmp")

    @pl.loop(0, rows // SUB)
    def _(g):
        band = pl.ds(pl.multiple_of(g * SUB, SUB), SUB)
        for r, rnd in enumerate(rounds):
            first = source_block(io, cmp, rnd) * 2
            for h in range(2):
                at = first + h
                index = lane_ref[band, pl.ds(pl.multiple_of(at * LANES, LANES), LANES)]
                for f in range(fields):
                    value = pieces[r][f, band, h * LANES : (h + 1) * LANES]
                    turned[f, at, band, :] = lane_gather(value, index) * (1.0 / (STEPS + 1.0))


def moved_chunks(turned, move_ref, fs, band, wide):
    chunks = turned.shape[1]
    level = [{} for _ in range(STAGES + 1)]

    def settle(bit, k):
        if bit == STAGES:
            return
        amount = 1 << bit
        for at in (k - amount, k):
            if at < 0 or at in level[bit + 1] or (at + amount < chunks and at == k):
                continue
            value = level[bit].pop(at)
            if at + amount < chunks:
                arrive = move_ref[bit, band, at * LANES : (at + 1) * LANES] != 0
                near = level[bit][at + amount]
                value = [jnp.where(arrive, n, v) for n, v in zip(near, value)]
            level[bit + 1][at] = value
            settle(bit + 1, at)

    done = 0
    for k in range(chunks):
        level[0][k] = [turned[f, k, band, :] for f in fs]
        settle(0, k)
        while done < wide and done in level[STAGES]:
            yield done, level[STAGES].pop(done)
            level[STAGES][done] = None
            done += 1


def pack_kernel(turned, move_ref, count_ref, old_ref, new_ref, sum_ref, out, acc, sem):
    fields, rows, width = old_ref.shape
    groups = rows // SUB
    wide = width // LANES
    lane = lax.broadcasted_iota(jnp.int32, (SUB, LANES), 1)
    acc[...] = jnp.zeros_like(acc)

    def copy_out(g, slot, f0):
        fs, band = pl.ds(f0, SHARE), pl.ds(pl.multiple_of(g * SUB, SUB), SUB)
        return pltpu.make_async_copy(
            out.at[slot, fs], new_ref.at[fs, band, :], sem.at[slot, f0 // SHARE]
        )

    @pl.loop(0, groups)
    def _(g):
        slot = lax.rem(g, 2)
        band = pl.ds(pl.multiple_of(g * SUB, SUB), SUB)

        left = count_ref[band, :] - lane

        @pl.loop(0, fields, step=SHARE)
        def _(f0):
            fs = [f0 + j for j in range(SHARE)]

            @pl.when(g >= 2)
            def _():
                copy_out(g - 2, slot, f0).wait()

            squares = [acc[f] for f in fs]
            for k, values in moved_chunks(turned, move_ref, fs, band, wide):
                valid = left > k * LANES
                cut = slice(k * LANES, (k + 1) * LANES)
                for j, f in enumerate(fs):
                    mean = jnp.where(valid, old_ref[f, band, cut] + values[j], 0.0)
                    out[slot, f, :, cut] = mean
                    squares[j] = squares[j] + mean * mean
            for j, f in enumerate(fs):
                acc[f] = squares[j]
            copy_out(g, slot, f0).start()

    row = lax.broadcasted_iota(jnp.int32, (SUB, LANES), 0)
    total = jnp.zeros((SUB, LANES), jnp.float32)
    for f in range(fields):
        total = jnp.where(row == f, jnp.sum(acc[f], axis=0, keepdims=True), total)
    ocean = jnp.zeros_like(lane)
    for g in range(groups):
        ocean = ocean + count_ref[g * SUB : (g + 1) * SUB, :]
    ocean = jnp.where(lane == 0, ocean, 0).astype(jnp.float32)
    total = jnp.where(row == fields, jnp.sum(ocean, axis=0, keepdims=True), total)
    for p in range(sum_ref.shape[0]):
        sum_ref[p] = total
    for g in range(groups - 2, groups):
        for f0 in range(0, fields, SHARE):
            copy_out(g, g % 2, f0).wait()


def finish_kernel(part_ref, rms_ref):
    fields = rms_ref.shape[1]
    total = part_ref[0]
    for p in range(1, part_ref.shape[0]):
        total = total + part_ref[p]
    level = jnp.sum(total, axis=1, keepdims=True)
    rms = jnp.sqrt(level / level[fields : fields + 1] + 1e-06)
    row = lax.broadcasted_iota(jnp.int32, (SUB, LANES), 0)
    lane = lax.broadcasted_iota(jnp.int32, (SUB, LANES), 1)
    flat = jnp.sum(jnp.where(row == lane, rms, 0.0), axis=0, keepdims=True)
    rms_ref[...] = flat[:, :fields]


VMEM = pl.BlockSpec(memory_space=pltpu.VMEM)


def cut(rounds, fields, grant):
    nfield, _, nrow, ncol = fields.shape
    piece = jax.ShapeDtypeStruct((nfield, nrow // 2, ncol), jnp.float32)
    return pl.pallas_call(
        functools.partial(cut_kernel, rounds),
        out_shape=(piece,) * len(rounds),
        in_specs=[pl.BlockSpec(memory_space=pltpu.HBM)],
        out_specs=(VMEM,) * len(rounds),
        scratch_shapes=[pltpu.SemaphoreType.DMA((len(rounds),))],
        compiler_params=pltpu.CompilerParams(vmem_limit_bytes=grant << 18),
        cost_estimate=pl.CostEstimate(
            flops=0, bytes_accessed=800_000 * len(rounds), transcendentals=0
        ),
        name="cut",
    )(fields)


def row_indices(mask, old):
    rows, ncol = mask.shape
    return pl.pallas_call(
        index_kernel,
        out_shape=(
            jax.ShapeDtypeStruct((rows, ncol), jnp.int32),
            jax.ShapeDtypeStruct((STAGES, rows, ncol), jnp.int32),
            jax.ShapeDtypeStruct((rows, LANES), jnp.int32),
            jax.ShapeDtypeStruct(old.shape, jnp.float32),
        ),
        in_specs=[VMEM, VMEM],
        out_specs=(VMEM,) * 4,
        scratch_shapes=[pltpu.VMEM((rows, ncol), jnp.int32)],
        compiler_params=pltpu.CompilerParams(vmem_limit_bytes=3 << 20),
        cost_estimate=pl.CostEstimate(flops=20_000_000, bytes_accessed=12 << 20, transcendentals=0),
        name="row_indices",
    )(mask, old)


def turn(rounds, lanes, pieces, turned):
    fields, rows, _ = pieces[0].shape
    shape = jax.ShapeDtypeStruct((fields, lanes.shape[1] // LANES, rows, LANES), jnp.float32)
    before = [] if turned is None else [turned]
    return pl.pallas_call(
        functools.partial(turn_kernel, rounds, len(before)),
        out_shape=shape,
        in_specs=[VMEM] * (1 + len(pieces) + len(before)),
        out_specs=VMEM,
        input_output_aliases={1 + len(pieces): 0} if before else {},
        compiler_params=pltpu.CompilerParams(vmem_limit_bytes=2 << 20),
        cost_estimate=pl.CostEstimate(
            flops=1_000_000 * len(pieces), bytes_accessed=800_000 * len(pieces), transcendentals=0
        ),
        name="turn",
    )(lanes, *pieces, *before)


def pack(turned, moves, counts, old, copies=16):
    fields, _, width = old.shape
    return pl.pallas_call(
        pack_kernel,
        out_shape=(
            jax.ShapeDtypeStruct(old.shape, jnp.float32),
            jax.ShapeDtypeStruct((copies, SUB, LANES), jnp.float32),
        ),
        in_specs=[VMEM] * 4,
        out_specs=(pl.BlockSpec(memory_space=pltpu.HBM), VMEM),
        scratch_shapes=[
            pltpu.VMEM((2, fields, SUB, width), jnp.float32),
            pltpu.VMEM((fields, SUB, LANES), jnp.float32),
            pltpu.SemaphoreType.DMA((2, fields // SHARE)),
        ],
        compiler_params=pltpu.CompilerParams(vmem_limit_bytes=6 << 20),
        cost_estimate=pl.CostEstimate(flops=40_000_000, bytes_accessed=16 << 20, transcendentals=0),
        name="pack",
    )(turned, moves, counts, old)


def finish(part, fields):
    return pl.pallas_call(
        finish_kernel,
        out_shape=jax.ShapeDtypeStruct((1, fields), jnp.float32),
        in_specs=[VMEM],
        out_specs=VMEM,
        compiler_params=pltpu.CompilerParams(vmem_limit_bytes=1 << 20),
        name="finish",
    )(part)


def on_device(fields, mean_old, land_mask):
    nfield = fields.shape[0]
    cuts = []
    for low, high, grant in zip(CUTS, CUTS[1:], GRANTS):
        cuts += cut(ROUNDS[low:high], fields, grant)
    pieces = []
    for k, rnd in enumerate(ROUNDS):
        pieces.append(lax.ppermute(cuts[k], ("io", "cmp"), pairs_of(rnd)))
    lanes, moves, counts, share = row_indices(land_mask[0], mean_old[:, 0])
    turned = None
    for low, high in zip(TURNS, TURNS[1:]):
        turned = turn(ROUNDS[low:high], lanes, pieces[low:high], turned)
    mean_new, part = pack(turned, moves, counts, share, lax.axis_size("io"))
    rms = finish(lax.all_to_all(part, "io", 0, 0, tiled=True), nfield)
    return mean_new[:, None], rms.T


def solution(mesh):
    in_specs = (P(None, None, "cmp", "io"), P(None, "cmp", "io", None), P("cmp", "io", None))
    out_specs = (P(None, "cmp", "io", None), P(None, "cmp"))
    return jax.shard_map(
        on_device, mesh=mesh, in_specs=in_specs, out_specs=out_specs, check_vma=False
    )
```

```python
import functools
import itertools

import jax
import jax.numpy as jnp
from jax import lax
from jax.experimental import pallas as pl
from jax.experimental.pallas import tpu as pltpu
from jax.sharding import PartitionSpec as P


STEPS = 3
LANES = 128
SUB = 8
ROUNDS = tuple(
    (pair[j ^ kc], ks, kc)
    for pair in ((1, 3), (0, 2))
    for ks in (1, 0)
    for kc in (0, 1)
    for j in (0, 1)
)
STAGES = 5
TURNS = ((0, 1, 2, 3, 4, 5, 8, 9), (6, 7, 10, 11), (12, 13), (14, 15))
CUTS = (0, 4, 16)
GRANTS = (204, 192)
SHARE = 3


def target_of(i, c, rnd):
    kx, ks, kc = rnd
    z, y, x = i >> 2, i & 3, c >> 1
    level = ((x - z + kx) & 3) * 2 + ((y >> 1) ^ kc)
    half = (y & 1) ^ ks
    return level, half


def source_block(b, l, rnd):
    kx, ks, kc = rnd
    z1, y1, x1, core1 = b >> 2, b & 3, l >> 1, l & 1
    z = (z1 - x1 + kx) & 3
    return z * 4 + (core1 ^ kc) * 2 + ((y1 & 1) ^ ks)


def pairs_of(rnd):
    out = []
    for i in range(16):
        for c in range(8):
            level, half = target_of(i, c, rnd)
            out.append((i * 8 + c, (2 * c + half) * 8 + level))
    return out


def cut_kernel(rounds, fields_ref, *refs):
    outs, sem = refs[: len(rounds)], refs[len(rounds)]
    rows = outs[0].shape[1]
    i, c = lax.axis_index("io"), lax.axis_index("cmp")
    copies = []
    for r, rnd in enumerate(rounds):
        level, half = target_of(i, c, rnd)
        band = pl.ds(pl.multiple_of(half * rows, rows), rows)
        copies.append(
            pltpu.make_async_copy(fields_ref.at[:, level, band, :], outs[r], sem.at[r])
        )
    for copy in copies:
        copy.start()
    for copy in copies:
        copy.wait()


def lane_gather(values, index):
    return jnp.take_along_axis(values, index, axis=1, mode="promise_in_bounds")


def index_kernel(mask_ref, old_ref, lane_ref, move_ref, count_ref, share_ref, upto_ref, total_ref):
    rows, ncol = mask_ref.shape
    chunks = ncol // LANES
    before = lax.broadcasted_iota(jnp.int32, (LANES, LANES), 0) <= lax.broadcasted_iota(
        jnp.int32, (LANES, LANES), 1
    )
    upper = before.astype(jnp.bfloat16)
    ones = jnp.ones((LANES, LANES), jnp.bfloat16)
    for k in range(chunks):
        cut = slice(k * LANES, (k + 1) * LANES)
        mb = mask_ref[:, cut].astype(jnp.float32).astype(jnp.bfloat16)
        upto = jnp.dot(mb, upper, preferred_element_type=jnp.float32)
        total = jnp.dot(mb, ones, preferred_element_type=jnp.float32)
        upto_ref[:, cut] = upto.astype(jnp.int32)
        total_ref[:, cut] = total.astype(jnp.int32)
    lane = lax.broadcasted_iota(jnp.int32, (SUB, LANES), 1)

    @pl.loop(0, rows // SUB)
    def _(g):
        band = pl.ds(pl.multiple_of(g * SUB, SUB), SUB)
        start = jnp.zeros((SUB, LANES), jnp.int32)
        dist = []
        for k in range(chunks):
            cut = slice(k * LANES, (k + 1) * LANES)
            total = total_ref[band, cut]
            ocean = mask_ref[band, cut] == 1
            state = jnp.where(ocean, ((lane - upto_ref[band, cut] + 1) << 7) | lane, 0)
            for bit in range(7):
                moving = jnp.where((state & (128 << bit)) != 0, state, 0)
                state = (state ^ moving) | pltpu.roll(moving, LANES - (1 << bit), 1)
            rank = (lane - start) & (LANES - 1)
            lane_ref[band, cut] = lane_gather(state & (LANES - 1), rank)
            chunk = (start + rank) >> 7
            dist.append(jnp.where(rank < total, k - chunk, 0))
            start = start + total
        count_ref[band, :] = start
        for bit in range(STAGES):
            amount = 1 << bit
            for k in range(chunks):
                stay = jnp.where((dist[k] & amount) != 0, 0, dist[k])
                if k + amount < chunks:
                    there = dist[k + amount]
                    arrive = there & amount
                    move_ref[bit, band, k * LANES : (k + 1) * LANES] = arrive
                    stay = jnp.where(arrive != 0, there, stay)
                dist[k] = stay
        for f in range(old_ref.shape[0]):
            share_ref[f, band, :] = old_ref[f, band, :] * (STEPS / (STEPS + 1.0))


def turn_kernel(rounds, reuse, lane_ref, *refs):
    pieces = refs[: len(rounds)]
    turned = refs[len(rounds) + reuse]
    fields, rows, _ = pieces[0].shape
    io, cmp = lax.axis_index("io"), lax.axis_index("cmp")

    wide = max(1, 16 // len(rounds))

    @pl.loop(0, rows // SUB, step=wide)
    def _(g0):
        for r, rnd in enumerate(rounds):
            first = source_block(io, cmp, rnd) * 2
            for h, j in itertools.product(range(2), range(wide)):
                at = first + h
                band = pl.ds(pl.multiple_of((g0 + j) * SUB, SUB), SUB)
                index = lane_ref[band, pl.ds(pl.multiple_of(at * LANES, LANES), LANES)]
                for f in range(fields):
                    value = pieces[r][f, band, h * LANES : (h + 1) * LANES]
                    turned[f, at, band, :] = lane_gather(value, index) * (1.0 / (STEPS + 1.0))


def moved_chunks(turned, move_ref, fs, band, wide):
    chunks = turned.shape[1]
    level = [{} for _ in range(STAGES + 1)]

    def settle(bit, k):
        if bit == STAGES:
            return
        amount = 1 << bit
        for at in (k - amount, k):
            if at < 0 or at in level[bit + 1] or (at + amount < chunks and at == k):
                continue
            value = level[bit].pop(at)
            if at + amount < chunks:
                arrive = move_ref[bit, band, at * LANES : (at + 1) * LANES] != 0
                near = level[bit][at + amount]
                value = [jnp.where(arrive, n, v) for n, v in zip(near, value)]
            level[bit + 1][at] = value
            settle(bit + 1, at)

    done = 0
    for k in range(chunks):
        level[0][k] = [turned[f, k, band, :] for f in fs]
        settle(0, k)
        while done < wide and done in level[STAGES]:
            yield done, level[STAGES].pop(done)
            level[STAGES][done] = None
            done += 1


def pack_kernel(turned, move_ref, count_ref, old_ref, new_ref, sum_ref, out, acc, sem):
    fields, rows, width = old_ref.shape
    groups = rows // SUB
    wide = width // LANES
    lane = lax.broadcasted_iota(jnp.int32, (SUB, LANES), 1)
    acc[...] = jnp.zeros_like(acc)

    def copy_out(g, f0):
        fs, band = pl.ds(f0, SHARE), pl.ds(pl.multiple_of(g * SUB, SUB), SUB)
        return pltpu.make_async_copy(
            out.at[fs, band, :], new_ref.at[fs, band, :], sem.at[g, f0 // SHARE]
        )

    @pl.loop(0, groups)
    def _(g):
        band = pl.ds(pl.multiple_of(g * SUB, SUB), SUB)

        left = count_ref[band, :] - lane

        @pl.loop(0, fields, step=SHARE)
        def _(f0):
            fs = [f0 + j for j in range(SHARE)]
            squares = [acc[f] for f in fs]
            for k, values in moved_chunks(turned, move_ref, fs, band, wide):
                valid = left > k * LANES
                cut = slice(k * LANES, (k + 1) * LANES)
                for j, f in enumerate(fs):
                    mean = jnp.where(valid, old_ref[f, band, cut] + values[j], 0.0)
                    out[f, band, cut] = mean
                    squares[j] = squares[j] + mean * mean
            for j, f in enumerate(fs):
                acc[f] = squares[j]
            copy_out(g, f0).start()

    row = lax.broadcasted_iota(jnp.int32, (SUB, LANES), 0)
    total = jnp.zeros((SUB, LANES), jnp.float32)
    for f in range(fields):
        total = jnp.where(row == f, jnp.sum(acc[f], axis=0, keepdims=True), total)
    ocean = jnp.zeros_like(lane)
    for g in range(groups):
        ocean = ocean + count_ref[g * SUB : (g + 1) * SUB, :]
    ocean = jnp.where(lane == 0, ocean, 0).astype(jnp.float32)
    total = jnp.where(row == fields, jnp.sum(ocean, axis=0, keepdims=True), total)
    for p in range(sum_ref.shape[0]):
        sum_ref[p] = total
    for g in range(groups):
        for f0 in range(0, fields, SHARE):
            copy_out(g, f0).wait()


def finish_kernel(part_ref, rms_ref):
    fields = rms_ref.shape[1]
    total = part_ref[0]
    for p in range(1, part_ref.shape[0]):
        total = total + part_ref[p]
    level = jnp.sum(total, axis=1, keepdims=True)
    rms = jnp.sqrt(level / level[fields : fields + 1] + 1e-06)
    row = lax.broadcasted_iota(jnp.int32, (SUB, LANES), 0)
    lane = lax.broadcasted_iota(jnp.int32, (SUB, LANES), 1)
    flat = jnp.sum(jnp.where(row == lane, rms, 0.0), axis=0, keepdims=True)
    rms_ref[...] = flat[:, :fields]


VMEM = pl.BlockSpec(memory_space=pltpu.VMEM)


def cut(rounds, fields, grant):
    nfield, _, nrow, ncol = fields.shape
    piece = jax.ShapeDtypeStruct((nfield, nrow // 2, ncol), jnp.float32)
    return pl.pallas_call(
        functools.partial(cut_kernel, rounds),
        out_shape=(piece,) * len(rounds),
        in_specs=[pl.BlockSpec(memory_space=pltpu.HBM)],
        out_specs=(VMEM,) * len(rounds),
        scratch_shapes=[pltpu.SemaphoreType.DMA((len(rounds),))],
        compiler_params=pltpu.CompilerParams(vmem_limit_bytes=grant << 18),
        cost_estimate=pl.CostEstimate(
            flops=0, bytes_accessed=800_000 * len(rounds), transcendentals=0
        ),
        name="cut",
    )(fields)


def row_indices(mask, old):
    rows, ncol = mask.shape
    return pl.pallas_call(
        index_kernel,
        out_shape=(
            jax.ShapeDtypeStruct((rows, ncol), jnp.int32),
            jax.ShapeDtypeStruct((STAGES, rows, ncol), jnp.int32),
            jax.ShapeDtypeStruct((rows, LANES), jnp.int32),
            jax.ShapeDtypeStruct(old.shape, jnp.float32),
        ),
        in_specs=[VMEM, VMEM],
        out_specs=(VMEM,) * 4,
        scratch_shapes=[pltpu.VMEM((rows, ncol), jnp.int32)] * 2,
        compiler_params=pltpu.CompilerParams(vmem_limit_bytes=4 << 20),
        cost_estimate=pl.CostEstimate(flops=20_000_000, bytes_accessed=12 << 20, transcendentals=0),
        name="row_indices",
    )(mask, old)


def turn(rounds, lanes, pieces, turned):
    fields, rows, _ = pieces[0].shape
    shape = jax.ShapeDtypeStruct((fields, lanes.shape[1] // LANES, rows, LANES), jnp.float32)
    before = [] if turned is None else [turned]
    return pl.pallas_call(
        functools.partial(turn_kernel, rounds, len(before)),
        out_shape=shape,
        in_specs=[VMEM] * (1 + len(pieces) + len(before)),
        out_specs=VMEM,
        input_output_aliases={1 + len(pieces): 0} if before else {},
        compiler_params=pltpu.CompilerParams(vmem_limit_bytes=2 << 20),
        cost_estimate=pl.CostEstimate(
            flops=1_000_000 * len(pieces), bytes_accessed=800_000 * len(pieces), transcendentals=0
        ),
        name="turn",
    )(lanes, *pieces, *before)


def pack(turned, moves, counts, old, copies=16):
    fields, rows, width = old.shape
    return pl.pallas_call(
        pack_kernel,
        out_shape=(
            jax.ShapeDtypeStruct(old.shape, jnp.float32),
            jax.ShapeDtypeStruct((copies, SUB, LANES), jnp.float32),
        ),
        in_specs=[VMEM] * 4,
        out_specs=(pl.BlockSpec(memory_space=pltpu.HBM), VMEM),
        scratch_shapes=[
            pltpu.VMEM((fields, rows, width), jnp.float32),
            pltpu.VMEM((fields, SUB, LANES), jnp.float32),
            pltpu.SemaphoreType.DMA((rows // SUB, fields // SHARE)),
        ],
        compiler_params=pltpu.CompilerParams(vmem_limit_bytes=8 << 20),
        cost_estimate=pl.CostEstimate(flops=40_000_000, bytes_accessed=16 << 20, transcendentals=0),
        name="pack",
    )(turned, moves, counts, old)


def finish(part, fields):
    return pl.pallas_call(
        finish_kernel,
        out_shape=jax.ShapeDtypeStruct((1, fields), jnp.float32),
        in_specs=[VMEM],
        out_specs=VMEM,
        compiler_params=pltpu.CompilerParams(vmem_limit_bytes=1 << 20),
        name="finish",
    )(part)


def on_device(fields, mean_old, land_mask):
    nfield = fields.shape[0]
    cuts = []
    for low, high, grant in zip(CUTS, CUTS[1:], GRANTS):
        cuts += cut(ROUNDS[low:high], fields, grant)
    pieces = []
    for k, rnd in enumerate(ROUNDS):
        pieces.append(lax.ppermute(cuts[k], ("io", "cmp"), pairs_of(rnd)))
    lanes, moves, counts, share = row_indices(land_mask[0], mean_old[:, 0])
    turned = None
    for taken in TURNS:
        rounds = tuple(ROUNDS[k] for k in taken)
        turned = turn(rounds, lanes, [pieces[k] for k in taken], turned)
    mean_new, part = pack(turned, moves, counts, share, lax.axis_size("io"))
    rms = finish(lax.all_to_all(part, "io", 0, 0, tiled=True), nfield)
    return mean_new[:, None], rms.T


def solution(mesh):
    in_specs = (P(None, None, "cmp", "io"), P(None, "cmp", "io", None), P("cmp", "io", None))
    out_specs = (P(None, "cmp", "io", None), P(None, "cmp"))
    return jax.shard_map(
        on_device, mesh=mesh, in_specs=in_specs, out_specs=out_specs, check_vma=False
    )
```
